32 devices in a mesh: row: 8 (over y, x, core), col: 4 (over z).
Axes of the slice: x: 2, y: 2, z: 4, core: 2. Of those that a mesh axis runs over, the one named last changes fastest.
Arguments:
- src_points: bfloat16 [8192, 256], P('row'), may hold values from -32 to 32, as said below
- tgt_points: bfloat16 [16384, 256], P(('col', 'row')), may hold values from -32 to 32, as said below
- log_src_mass: float32 [8192], P('row'), may hold values from -3 to 3
- log_tgt_mass: float32 [16384], P('col'), may hold values from -3 to 3
Outputs:
- src_potential: float32 [8192], P('row')
- tgt_potential: float32 [16384], P('col')
- mean_potentials: float32 [], replicated
The draws below stay inside these ranges and needn't reach their ends.
Inputs may be any that keep to these rules, and one draw needn't show every extreme that they name: `src_points`: point coordinates. `tgt_points`: point coordinates.
All inputs are finite; a program needn't handle non-finite values.
Results may differ from the reference program's by a relative error of at most 0.0003.
Values may be sent and summed in bfloat16 or wider, within the bound.
A program may use at most 64 MiB of HBM per device.

```python
import jax
import jax.numpy as jnp
from jax import lax

WIDTH = 256
TGT_DEV = 4096
ITERS = 3
SOURCES = 8192
TARGETS = 16384


def scaled_points(key, count):
    values = jnp.clip(jax.random.normal(jax.random.fold_in(key, 1), (count, WIDTH), jnp.float32), -8.0, 8.0)
    low, high = (0.5, 2.0)
    scales = jnp.exp(jax.random.uniform(jax.random.fold_in(key, 2), (count, 1), jnp.float32, jnp.log(low), jnp.log(high)))
    return values * scales


def target_cloud(key):
    points = scaled_points(key, TARGETS)
    groups = TARGETS // TGT_DEV
    offsets = jnp.clip(1.5 * jax.random.normal(jax.random.fold_in(key, 3), (groups, WIDTH), jnp.float32), -6.0, 6.0)
    points = points + jnp.repeat(offsets, TGT_DEV, axis=0)
    return jnp.clip(points, -32.0, 32.0)


def draw_tgt_points(key, part):
    return target_cloud(jax.random.fold_in(key, 71)).astype(jnp.bfloat16)


def draw_src_points(key, part):
    points = jnp.clip(scaled_points(jax.random.fold_in(key, 53), SOURCES), -32.0, 32.0)
    return points.astype(jnp.bfloat16)


def levels(stream_key, extent, pieces, least, high):
    level, own = 1.0, jax.random.fold_in(stream_key, 6)
    for dim, shards_of in pieces:
        steps = jnp.exp(jax.random.uniform(jax.random.fold_in(own, dim), (shards_of,), jnp.float32, least / len(pieces), high / len(pieces)))
        level = level * jnp.repeat(steps, extent[dim] // shards_of).reshape([-1 if axis == dim else 1 for axis in range(len(extent))])
    return level


def setup_inputs(seed: int = 0) -> dict:
    key_of = jax.random.split(jax.random.key(seed), 5)
    src_points = draw_src_points(jax.random.fold_in(key_of[4], 71), 0)
    tgt_points = draw_tgt_points(jax.random.fold_in(key_of[4], 71), 0)
    log_src_mass = jnp.clip(jax.random.uniform(key_of[2], (SOURCES,), jnp.float32, -3.0, 3.0) * levels(key_of[2], (SOURCES,), ((0, 8),), -0.4, 0.0), -3.0, 3.0)
    log_tgt_mass = jnp.clip(jax.random.uniform(key_of[3], (TARGETS,), jnp.float32, -3.0, 3.0) * levels(key_of[3], (TARGETS,), ((0, 4),), -0.4, 0.0), -3.0, 3.0)
    return {"src_points": src_points, "tgt_points": tgt_points, "log_src_mass": log_src_mass, "log_tgt_mass": log_tgt_mass}


entropy_weight = 0.1


def cost_block(points_a, squares_a, points_b, squares_b):
    product = lax.dot_general(points_a, points_b, (((1,), (1,)), ((), ())), preferred_element_type=jnp.float32)
    return (squares_a[:, None] + squares_b[None, :] - 2.0 * product) / points_a.shape[1]


def reference(src_points, tgt_points, log_src_mass, log_tgt_mass):
    sqx = jnp.sum(src_points.astype(jnp.float32) ** 2, axis=1)
    sqy = jnp.sum(tgt_points.astype(jnp.float32) ** 2, axis=1)
    blocks = SOURCES // min(1024, SOURCES)
    src_blocks = src_points.reshape(blocks, -1, WIDTH)
    sq_blocks = sqx.reshape(blocks, -1)
    mass_blocks = log_src_mass.reshape(blocks, -1)
    costs = lax.map(lambda item: cost_block(item[0], item[1], tgt_points, sqy), (src_blocks, sq_blocks))
    tgt_potential = jnp.zeros((TARGETS,), jnp.float32)
    src_potential = jnp.zeros((SOURCES,), jnp.float32)
    for step in range(ITERS):
        def source_rows(cost):
            terms = log_tgt_mass[None, :] + (tgt_potential[None, :] - cost) / entropy_weight
            top = jnp.max(terms, axis=1)
            return top + jnp.log(jnp.sum(jnp.exp(terms - top[:, None]), axis=1))

        src_potential = -entropy_weight * lax.map(source_rows, costs).reshape(-1)
        pot_blocks = src_potential.reshape(blocks, -1)

        def target_step(carry, item):
            cost, mass, pot = item
            terms = mass[:, None] + (pot[:, None] - cost) / entropy_weight
            block_top = jnp.max(terms, axis=0)
            block_sum = jnp.sum(jnp.exp(terms - block_top[None, :]), axis=0)
            top = jnp.maximum(carry[0], block_top)
            total = carry[1] * jnp.exp(carry[0] - top) + block_sum * jnp.exp(block_top - top)
            return (top, total), None

        start = (jnp.full((TARGETS,), -jnp.inf, jnp.float32), jnp.zeros((TARGETS,), jnp.float32))
        (top, total), unused = lax.scan(target_step, start, (costs, mass_blocks, pot_blocks))
        tgt_potential = -entropy_weight * (top + jnp.log(total))
    mean_potentials = jnp.mean(src_potential) + jnp.mean(tgt_potential)
    return src_potential, tgt_potential, mean_potentials
```

```python
import functools
import math

import jax
import jax.numpy as jnp
from jax import lax
from jax.experimental import pallas as pl
from jax.experimental.pallas import tpu as pltpu
from jax.sharding import PartitionSpec as P

ITERS = 3
entropy_weight = 0.1
LOG2E = math.log2(math.e)
SCALE = LOG2E / entropy_weight
LANES = 128
HIGHEST = lax.Precision.HIGHEST
MESH = pl.DeviceIdType.MESH


def to_col(row):
    return jnp.broadcast_to(row, (LANES, LANES)).T


def widen(col, width):
    return jnp.concatenate([col] * (width // LANES), axis=1)


def fold(x, op):
    parts = [x[:, k : k + LANES] for k in range(0, x.shape[1], LANES)]
    while len(parts) > 1:
        parts = [op(a, b) for a, b in zip(parts[::2], parts[1::2])] + parts[len(parts) & ~1 :]
    return parts[0]


def flip(index, bit):
    return index + bit - 2 * bit * (index // bit % 2)


def kernel(
    nrow, ncol, chunks,
    x_hbm, t_hbm, ls_ref, lm_ref,
    f_ref, g_ref, mean_ref,
    x_ref, gath, z_ref, pcol, mlane, glane, wlane, fbuf, gbuf, tbuf, hbuf,
    in_sem, blk_send, blk_recv, f_send, f_recv, g_send, g_recv, t_sem, h_sem,
):
    r, c = lax.axis_index("row"), lax.axis_index("col")
    sources, width = x_ref.shape
    targets = z_ref.shape[0]
    block = targets // nrow
    half = block // 2
    chunk = targets // chunks
    sub = min(256, block)

    load_t = pltpu.make_async_copy(t_hbm, gath.at[r], in_sem.at[0])
    load_x = pltpu.make_async_copy(x_hbm, x_ref, in_sem.at[1])
    load_t.start()
    load_x.start()

    barrier = pltpu.get_barrier_semaphore()
    for d in range(1, nrow):
        pl.semaphore_signal(barrier, inc=1, device_id=(lax.rem(r + d, nrow), c), device_id_type=MESH)
    for d in range(1, ncol):
        pl.semaphore_signal(barrier, inc=1, device_id=(r, lax.rem(c + d, ncol)), device_id_type=MESH)
    load_t.wait()
    pl.semaphore_wait(barrier, nrow + ncol - 2)

    sent = []

    def send_block(slot, part, to):
        rows = pl.ds(part * half, half)
        copy = pltpu.make_async_remote_copy(
            src_ref=gath.at[slot, rows],
            dst_ref=gath.at[slot, rows],
            send_sem=blk_send.at[len(sent)],
            recv_sem=blk_recv.at[slot, part],
            device_id=(to, c),
            device_id_type=MESH,
        )
        copy.start()
        sent.append(copy)

    def wait_block(slot, part):
        rows = pl.ds(part * half, half)
        pltpu.make_async_copy(gath.at[slot, rows], gath.at[slot, rows], blk_recv.at[slot, part]).wait()

    if nrow == 8:
        p1, px, py = flip(r, 1), flip(r, 2), flip(r, 4)
        send_block(r, 0, px)
        send_block(r, 1, py)
        send_block(r, 1, px)
        send_block(r, 0, py)
        send_block(r, 0, p1)
        send_block(r, 1, p1)
    else:
        for d in range(1, nrow):
            for part in range(2):
                send_block(r, part, lax.rem(r + d, nrow))

    load_x.wait()
    x32 = x_ref[...].astype(jnp.float32)
    qx = lax.dot_general(
        jnp.ones((8, width), jnp.float32), x32 * x32, (((1,), (1,)), ((), ())),
        precision=HIGHEST, preferred_element_type=jnp.float32,
    )[0:1] * (SCALE / width)
    ls2 = ls_ref[...] * LOG2E
    els = jnp.exp2(ls2)

    def row_block(slot, carry):
        def piece(k, carry):
            top, total = carry
            start = pl.multiple_of(slot * block + k * sub, sub)
            pts = gath[slot, pl.ds(pl.multiple_of(k * sub, sub), sub), :]
            product = lax.dot_general(
                pts, x_ref[...], (((1,), (1,)), ((), ())), preferred_element_type=jnp.float32
            )
            p32 = pts.astype(jnp.float32)
            sq = jnp.sum(p32 * p32, axis=1, keepdims=True) * (SCALE / width)
            cols = [
                to_col(lm_ref[:, pl.ds(pl.multiple_of(start + b, LANES), LANES)])
                for b in range(0, sub, LANES)
            ]
            shift = jnp.concatenate(cols, axis=0) * LOG2E - jnp.broadcast_to(sq, (sub, LANES))
            z = product * (2.0 * SCALE / width) + widen(shift, sources)
            z_ref[pl.ds(start, sub), :] = z
            new_top = jnp.maximum(top, jnp.max(z.reshape(sub // 8, 8, sources), axis=0))
            again = z_ref[pl.ds(start, sub), :].reshape(sub // 8, 8, sources)
            part = jnp.sum(jnp.exp2(again - new_top[None]), axis=0)
            return new_top, total * jnp.exp2(top - new_top) + part

        return lax.fori_loop(0, block // sub, piece, carry)

    carry = (jnp.full((8, sources), -3.0e38, jnp.float32), jnp.zeros((8, sources), jnp.float32))
    carry = row_block(r, carry)
    if nrow == 8:
        wait_block(p1, 0)
        wait_block(p1, 1)
        carry = row_block(p1, carry)
        wait_block(px, 0)
        send_block(px, 0, py)
        send_block(px, 0, p1)
        wait_block(py, 1)
        send_block(py, 1, px)
        send_block(py, 1, p1)
        wait_block(px, 1)
        send_block(px, 1, p1)
        wait_block(py, 0)
        send_block(py, 0, p1)
        pd = flip(px, 4)
        order = [px, py, flip(px, 1), flip(py, 1)]
        carry = row_block(px, carry)
        carry = row_block(py, carry)
        for slot in order[2:]:
            wait_block(slot, 0)
            wait_block(slot, 1)
            carry = row_block(slot, carry)
        for part in range(2):
            wait_block(pd, part)
            send_block(pd, part, p1)
        carry = row_block(pd, carry)
        last = flip(pd, 1)
        wait_block(last, 0)
        wait_block(last, 1)
        carry = row_block(last, carry)
    else:
        for d in range(1, nrow):
            slot = lax.rem(r + nrow - d, nrow)
            wait_block(slot, 0)
            wait_block(slot, 1)
            carry = row_block(slot, carry)

    def send_f(k, buf, send_sem, recv_sem):
        for d in range(1, ncol):
            pltpu.make_async_remote_copy(
                src_ref=buf.at[k, c], dst_ref=buf.at[k, c], send_sem=send_sem.at[k],
                recv_sem=recv_sem.at[k], device_id=(r, lax.rem(c + d, ncol)), device_id_type=MESH,
            ).start()

    def send_row(k, buf, send_sem, recv_sem):
        for d in range(1, nrow):
            pltpu.make_async_remote_copy(
                src_ref=buf.at[k, r], dst_ref=buf.at[k, r], send_sem=send_sem.at[k],
                recv_sem=recv_sem.at[k], device_id=(lax.rem(r + d, nrow), c), device_id_type=MESH,
            ).start()

    def wait_all(k, buf, sem):
        part = buf.at[k, pl.ds(0, buf.shape[1] - 1)]
        pltpu.make_async_copy(part, part, sem.at[k]).wait()

    def total_of(k, buf):
        return functools.reduce(lambda a, b: a + b, [buf[k, d] for d in range(buf.shape[1])])

    def lse_of(k, buf):
        parts = [buf[k, d] for d in range(buf.shape[1])]
        top = functools.reduce(jnp.maximum, parts)
        return top + jnp.log2(functools.reduce(lambda a, b: a + b, [jnp.exp2(p - top) for p in parts]))

    top8, total8 = carry
    top = jnp.max(top8, axis=0, keepdims=True)
    total = jnp.sum(total8 * jnp.exp2(top8 - top), axis=0, keepdims=True)
    fbuf[0, c] = top + jnp.log2(total)
    send_f(0, fbuf, f_send, f_recv)
    wait_all(0, fbuf, f_recv)
    first_f = -lse_of(0, fbuf)
    shift = ls2 + first_f

    def compact(start):
        rows = [
            jnp.sum(pcol[pl.ds(pl.multiple_of(start + b, LANES), LANES), :].T, axis=0, keepdims=True)
            for b in range(0, chunk, LANES)
        ]
        return jnp.concatenate(rows, axis=1)

    def col_first(k):
        start = pl.multiple_of(k * chunk, chunk)

        def piece(i, unused):
            rows = pl.ds(pl.multiple_of(start + i * LANES, LANES), LANES)
            high = jnp.max(fold(z_ref[rows, :] + shift, jnp.maximum), axis=1, keepdims=True)
            high = jnp.broadcast_to(high, (LANES, LANES))
            e = jnp.exp2(z_ref[rows, :] + shift - widen(high, sources))
            z_ref[rows, :] = e
            pcol[rows, :] = fold(e, jnp.add)
            lane = pl.ds(pl.multiple_of(start + i * LANES, LANES), LANES)
            mlane[:, lane] = high.T[0:1, :]
            return unused

        lax.fori_loop(0, chunk // LANES, piece, 0)
        lane = pl.ds(start, chunk)
        gbuf[k, r] = mlane[:, lane] + jnp.log2(compact(start))
        send_row(k, gbuf, g_send, g_recv)

    for k in range(chunks):
        col_first(k)

    def row_again(k, it, acc):
        slot = (it - 1) * chunks + k
        start = k * chunk
        lane = pl.ds(start, chunk)
        wait_all(slot, gbuf, g_recv)
        if it == 1:
            lse = lse_of(slot, gbuf)
            glane[:, lane] = lse
            wlane[0, :, lane] = jnp.exp2(mlane[:, lane] - lse)
            w = wlane[0, :, lane] * jnp.exp2(lm_ref[:, lane] * LOG2E)
            wlane[1, :, lane] = w
        else:
            w = wlane[1, :, lane] / total_of(slot, gbuf)
        wlane[2, :, lane] = w

        def piece(i, acc):
            lane = pl.ds(pl.multiple_of(start + i * LANES, LANES), LANES)
            wc = to_col(wlane[2, :, lane])
            product = z_ref[lane, :] * widen(wc, sources)
            return acc + jnp.sum(product.reshape(LANES // 8, 8, sources), axis=0)

        return lax.fori_loop(0, chunk // LANES, piece, acc)

    def col_again(k, it, u):
        start = k * chunk
        slot = it * chunks + k

        def piece(i, unused):
            rows = pl.ds(pl.multiple_of(start + i * LANES, LANES), LANES)
            pcol[rows, :] = fold(z_ref[rows, :] * u, jnp.add)
            return unused

        lax.fori_loop(0, chunk // LANES, piece, 0)
        gbuf[slot, r] = wlane[0, :, pl.ds(start, chunk)] * compact(start)
        send_row(slot, gbuf, g_send, g_recv)

    sources_all = sources * nrow
    targets_all = targets * ncol
    for it in range(1, ITERS):
        acc = jnp.zeros((8, sources), jnp.float32)
        for k in range(chunks):
            acc = row_again(k, it, acc)
        fbuf[it, c] = jnp.sum(acc, axis=0, keepdims=True)
        send_f(it, fbuf, f_send, f_recv)
        wait_all(it, fbuf, f_recv)
        rowsum = total_of(it, fbuf)
        u = els / rowsum
        if it == ITERS - 1:
            f = (first_f + qx + ls2 - jnp.log2(rowsum)) * (1.0 / SCALE)
            f_ref[...] = f
            tbuf[0, r] = jnp.broadcast_to(
                jnp.sum(f, axis=1, keepdims=True) * (1.0 / (sources_all * ncol)), (1, LANES)
            )
            send_row(0, tbuf, t_sem.at[0], t_sem.at[1])
        for k in range(chunks):
            col_again(k, it, u)

    acc = jnp.zeros((1, LANES), jnp.float32)
    for k in range(chunks):
        slot = (ITERS - 1) * chunks + k
        lane = pl.ds(k * chunk, chunk)
        wait_all(slot, gbuf, g_recv)
        g = (lm_ref[:, lane] * LOG2E - glane[:, lane] - jnp.log2(total_of(slot, gbuf))) * (1.0 / SCALE)
        g_ref[:, lane] = g
        acc = acc + fold(g, jnp.add)
    wait_all(0, tbuf, t_sem.at[1])
    hbuf[0, c] = total_of(0, tbuf) + jnp.broadcast_to(
        jnp.sum(acc, axis=1, keepdims=True) * (1.0 / targets_all), (1, LANES)
    )
    send_f(0, hbuf, h_sem.at[0], h_sem.at[1])
    wait_all(0, hbuf, h_sem.at[1])
    mean_ref[...] = total_of(0, hbuf)

    for copy in sent:
        copy.wait_send()
    for it in range(ITERS):
        wait_all(it, fbuf, f_send)
    for slot in range(ITERS * chunks):
        wait_all(slot, gbuf, g_send)
    wait_all(0, tbuf, t_sem.at[0])
    wait_all(0, hbuf, h_sem.at[0])


def body(nrow, ncol, src_points, tgt_points, log_src_mass, log_tgt_mass):
    sources, width = src_points.shape
    block = tgt_points.shape[0]
    targets = block * nrow
    chunks = 4
    chunk = targets // chunks
    f32 = jnp.float32
    vmem = pl.BlockSpec(memory_space=pltpu.VMEM)
    hbm = pl.BlockSpec(memory_space=pl.ANY)
    dma = pltpu.SemaphoreType.DMA
    sends = 14 if nrow == 8 else 2 * (nrow - 1)
    f, g, mean = pl.pallas_call(
        functools.partial(kernel, nrow, ncol, chunks),
        out_shape=(
            jax.ShapeDtypeStruct((1, sources), f32),
            jax.ShapeDtypeStruct((1, targets), f32),
            jax.ShapeDtypeStruct((1, LANES), f32),
        ),
        in_specs=[hbm, hbm, vmem, vmem],
        out_specs=(vmem, vmem, vmem),
        scratch_shapes=[
            pltpu.VMEM((sources, width), jnp.bfloat16),
            pltpu.VMEM((nrow, block, width), jnp.bfloat16),
            pltpu.VMEM((targets, sources), f32),
            pltpu.VMEM((targets, LANES), f32),
            pltpu.VMEM((1, targets), f32),
            pltpu.VMEM((1, targets), f32),
            pltpu.VMEM((3, 1, targets), f32),
            pltpu.VMEM((ITERS, ncol, 1, sources), f32),
            pltpu.VMEM((ITERS * chunks, nrow, 1, chunk), f32),
            pltpu.VMEM((1, nrow, 1, LANES), f32),
            pltpu.VMEM((1, ncol, 1, LANES), f32),
            dma((2,)),
            dma((sends,)),
            dma((nrow, 2)),
            dma((ITERS,)),
            dma((ITERS,)),
            dma((ITERS * chunks,)),
            dma((ITERS * chunks,)),
            dma((2, 1)),
            dma((2, 1)),
        ],
        compiler_params=pltpu.CompilerParams(
            collective_id=0, has_side_effects=True, vmem_limit_bytes=60 * 1024 * 1024
        ),
        name="sinkhorn",
    )(src_points, tgt_points, log_src_mass.reshape(1, -1), log_tgt_mass.reshape(1, -1))
    return f.reshape(-1), g.reshape(-1), mean[0, 0]


def solution(mesh):
    return jax.shard_map(
        functools.partial(body, mesh.shape["row"], mesh.shape["col"]),
        mesh=mesh,
        in_specs=(P("row", None), P(("col", "row"), None), P("row"), P("col")),
        out_specs=(P("row"), P("col"), P()),
        check_vma=False,
    )
```

```python
import functools
import math

import jax
import jax.numpy as jnp
from jax import lax
from jax.experimental import pallas as pl
from jax.experimental.pallas import tpu as pltpu
from jax.sharding import PartitionSpec as P

ITERS = 3
entropy_weight = 0.1
LOG2E = math.log2(math.e)
SCALE = LOG2E / entropy_weight
LANES = 128
HIGHEST = lax.Precision.HIGHEST
MESH = pl.DeviceIdType.MESH


def to_col(row):
    return jnp.broadcast_to(row, (LANES, LANES)).T


def widen(col, width):
    return jnp.concatenate([col] * (width // LANES), axis=1)


def fold(x, op):
    parts = [x[:, k : k + LANES] for k in range(0, x.shape[1], LANES)]
    while len(parts) > 1:
        parts = [op(a, b) for a, b in zip(parts[::2], parts[1::2])] + parts[len(parts) & ~1 :]
    return parts[0]


def flip(index, bit):
    return index + bit - 2 * bit * (index // bit % 2)


def kernel(
    nrow, ncol, chunks,
    x_hbm, t_hbm, ls_ref, lm_ref,
    f_ref, g_ref, mean_ref,
    x_ref, gath, z_ref, mlane, glane, wlane, fbuf, gbuf, tbuf, hbuf,
    in_sem, blk_send, blk_recv, f_send, f_recv, g_send, g_recv, t_sem, h_sem,
):
    r, c = lax.axis_index("row"), lax.axis_index("col")
    sources, width = x_ref.shape
    targets = z_ref.shape[0]
    block = targets // nrow
    half = block // 2
    chunk = targets // chunks
    wide, wide_first = min(512, chunk), min(256, chunk)
    sub = min(256, half)

    load_t = pltpu.make_async_copy(t_hbm, gath.at[r], in_sem.at[0])
    load_x = pltpu.make_async_copy(x_hbm, x_ref, in_sem.at[1])
    load_t.start()
    load_x.start()

    barrier = pltpu.get_barrier_semaphore()
    for d in range(1, ncol):
        pl.semaphore_signal(barrier, inc=1, device_id=(r, lax.rem(c + d, ncol)), device_id_type=MESH)
    for d in range(1, nrow):
        pl.semaphore_signal(barrier, inc=1, device_id=(lax.rem(r + d, nrow), c), device_id_type=MESH)
    load_t.wait()
    pl.semaphore_wait(barrier, nrow + ncol - 2)

    sent = []

    def send_block(slot, part, to):
        rows = pl.ds(part * half, half)
        copy = pltpu.make_async_remote_copy(
            src_ref=gath.at[slot, rows],
            dst_ref=gath.at[slot, rows],
            send_sem=blk_send.at[len(sent)],
            recv_sem=blk_recv.at[slot, part],
            device_id=(to, c),
            device_id_type=MESH,
        )
        copy.start()
        sent.append(copy)

    def wait_block(slot, part):
        rows = pl.ds(part * half, half)
        pltpu.make_async_copy(gath.at[slot, rows], gath.at[slot, rows], blk_recv.at[slot, part]).wait()

    if nrow == 8:
        p1, px, py = flip(r, 1), flip(r, 2), flip(r, 4)
        send_block(r, 0, px)
        send_block(r, 1, py)
        send_block(r, 1, px)
        send_block(r, 0, py)
        send_block(r, 0, p1)
        send_block(r, 1, p1)
    else:
        for d in range(1, nrow):
            for part in range(2):
                send_block(r, part, lax.rem(r + d, nrow))

    load_x.wait()
    x32 = x_ref[...].astype(jnp.float32)
    qx = lax.dot_general(
        jnp.ones((8, width), jnp.float32), x32 * x32, (((1,), (1,)), ((), ())),
        precision=HIGHEST, preferred_element_type=jnp.float32,
    )[0:1] * (SCALE / width)
    ls2 = ls_ref[...] * LOG2E
    els = jnp.exp2(ls2)

    def row_half(slot, part, carry):
        base = part * half

        def piece(k, carry):
            top, total = carry
            start = pl.multiple_of(slot * block + base + k * sub, sub)
            pts = gath[slot, pl.ds(pl.multiple_of(base + k * sub, sub), sub), :]
            product = lax.dot_general(
                pts, x_ref[...], (((1,), (1,)), ((), ())), preferred_element_type=jnp.float32
            )
            p32 = pts.astype(jnp.float32)
            sq = jnp.sum(p32 * p32, axis=1, keepdims=True) * (SCALE / width)
            cols = [
                to_col(lm_ref[:, pl.ds(pl.multiple_of(start + b, LANES), LANES)])
                for b in range(0, sub, LANES)
            ]
            shift = jnp.concatenate(cols, axis=0) * LOG2E - jnp.broadcast_to(sq, (sub, LANES))
            z = product * (2.0 * SCALE / width) + widen(shift, sources)
            z_ref[pl.ds(start, sub), :] = z
            new_top = jnp.maximum(top, jnp.max(z.reshape(sub // 8, 8, sources), axis=0))
            again = z_ref[pl.ds(start, sub), :].reshape(sub // 8, 8, sources)
            part = jnp.sum(jnp.exp2(again - new_top[None]), axis=0)
            return new_top, total * jnp.exp2(top - new_top) + part

        return lax.fori_loop(0, half // sub, piece, carry)

    carry = (jnp.full((8, sources), -3.0e38, jnp.float32), jnp.zeros((8, sources), jnp.float32))
    def arrived(slot, part, carry, *onward):
        wait_block(slot, part)
        for to in onward:
            send_block(slot, part, to)
        return row_half(slot, part, carry)

    carry = row_half(r, 1, row_half(r, 0, carry))
    if nrow == 8:
        carry = arrived(p1, 0, carry)
        carry = arrived(p1, 1, carry)
        wait_block(px, 0)
        send_block(px, 0, py)
        send_block(px, 0, p1)
        wait_block(py, 1)
        send_block(py, 1, px)
        send_block(py, 1, p1)
        carry = row_half(px, 0, carry)
        carry = row_half(py, 1, carry)
        px1, py1, pd = flip(px, 1), flip(py, 1), flip(px, 4)
        carry = arrived(px1, 0, carry)
        carry = arrived(px, 1, carry, p1)
        carry = arrived(py, 0, carry, p1)
        carry = arrived(py1, 1, carry)
        carry = arrived(px1, 1, carry)
        for part in range(2):
            wait_block(pd, part)
            send_block(pd, part, p1)
        carry = arrived(py1, 0, carry)
        carry = row_half(pd, 0, carry)
        carry = row_half(pd, 1, carry)
        last = flip(pd, 1)
        carry = arrived(last, 0, carry)
        carry = arrived(last, 1, carry)
    else:
        for d in range(1, nrow):
            slot = lax.rem(r + nrow - d, nrow)
            for part in range(2):
                carry = arrived(slot, part, carry)

    def send_f(k, buf, send_sem, recv_sem):
        for d in range(1, ncol):
            pltpu.make_async_remote_copy(
                src_ref=buf.at[k, c], dst_ref=buf.at[k, c], send_sem=send_sem.at[k],
                recv_sem=recv_sem.at[k], device_id=(r, lax.rem(c + d, ncol)), device_id_type=MESH,
            ).start()

    def send_row(k, buf, send_sem, recv_sem):
        for d in range(1, nrow):
            pltpu.make_async_remote_copy(
                src_ref=buf.at[k, r], dst_ref=buf.at[k, r], send_sem=send_sem.at[k],
                recv_sem=recv_sem.at[k], device_id=(lax.rem(r + d, nrow), c), device_id_type=MESH,
            ).start()

    def wait_all(k, buf, sem):
        part = buf.at[k, pl.ds(0, buf.shape[1] - 1)]
        pltpu.make_async_copy(part, part, sem.at[k]).wait()

    def total_of(k, buf):
        return functools.reduce(lambda a, b: a + b, [buf[k, d] for d in range(buf.shape[1])])

    def lse_of(k, buf):
        parts = [buf[k, d] for d in range(buf.shape[1])]
        top = functools.reduce(jnp.maximum, parts)
        return top + jnp.log2(functools.reduce(lambda a, b: a + b, [jnp.exp2(p - top) for p in parts]))

    top8, total8 = carry
    top = jnp.max(top8, axis=0, keepdims=True)
    total = jnp.sum(total8 * jnp.exp2(top8 - top), axis=0, keepdims=True)
    fbuf[0, c] = top + jnp.log2(total)
    send_f(0, fbuf, f_send, f_recv)
    wait_all(0, fbuf, f_recv)
    first_f = -lse_of(0, fbuf)
    shift = ls2 + first_f

    def sum_rows(p):
        return jnp.sum(p.T, axis=0, keepdims=True)

    def col_first(k):
        start = k * chunk

        def piece(i, unused):
            base = pl.multiple_of(i * wide_first, wide_first)
            for b in range(0, wide_first, LANES):
                rows = pl.ds(pl.multiple_of(start + base + b, LANES), LANES)
                high = jnp.max(fold(z_ref[rows, :] + shift, jnp.maximum), axis=1, keepdims=True)
                high = jnp.broadcast_to(high, (LANES, LANES))
                e = jnp.exp2(z_ref[rows, :] + shift - widen(high, sources))
                z_ref[rows, :] = e
                row = high.T[0:1, :]
                mlane[:, rows] = row
                lane = pl.ds(pl.multiple_of(base + b, LANES), LANES)
                gbuf[k, r, :, lane] = row + jnp.log2(sum_rows(fold(e, jnp.add)))
            return unused

        lax.fori_loop(0, chunk // wide_first, piece, 0)
        send_row(k, gbuf, g_send, g_recv)

    for k in range(chunks):
        col_first(k)

    def row_again(k, it, acc):
        slot = (it - 1) * chunks + k
        start = k * chunk
        lane = pl.ds(start, chunk)
        wait_all(slot, gbuf, g_recv)
        if it == 1:
            lse = lse_of(slot, gbuf)
            glane[:, lane] = lse
            wlane[0, :, lane] = jnp.exp2(mlane[:, lane] - lse)
            w = wlane[0, :, lane] * jnp.exp2(lm_ref[:, lane] * LOG2E)
            wlane[1, :, lane] = w
        else:
            w = wlane[1, :, lane] / total_of(slot, gbuf)
        wlane[2, :, lane] = w

        def piece(i, acc):
            for b in range(0, wide, LANES):
                lane = pl.ds(pl.multiple_of(start + i * wide + b, LANES), LANES)
                wc = to_col(wlane[2, :, lane])
                product = z_ref[lane, :] * widen(wc, sources)
                acc = acc + jnp.sum(product.reshape(LANES // 8, 8, sources), axis=0)
            return acc

        return lax.fori_loop(0, chunk // wide, piece, acc)

    def col_again(k, it, u):
        start = k * chunk
        slot = it * chunks + k

        def piece(i, unused):
            base = pl.multiple_of(i * wide, wide)
            for b in range(0, wide, LANES):
                rows = pl.ds(pl.multiple_of(start + base + b, LANES), LANES)
                lane = pl.ds(pl.multiple_of(base + b, LANES), LANES)
                sums = sum_rows(fold(z_ref[rows, :] * u, jnp.add))
                gbuf[slot, r, :, lane] = wlane[0, :, rows] * sums
            return unused

        lax.fori_loop(0, chunk // wide, piece, 0)
        send_row(slot, gbuf, g_send, g_recv)

    sources_all = sources * nrow
    targets_all = targets * ncol
    for it in range(1, ITERS):
        acc = jnp.zeros((8, sources), jnp.float32)
        for k in range(chunks):
            acc = row_again(k, it, acc)
        fbuf[it, c] = jnp.sum(acc, axis=0, keepdims=True)
        send_f(it, fbuf, f_send, f_recv)
        wait_all(it, fbuf, f_recv)
        rowsum = total_of(it, fbuf)
        u = els / rowsum
        if it == ITERS - 1:
            f = (first_f + qx + ls2 - jnp.log2(rowsum)) * (1.0 / SCALE)
            f_ref[...] = f
            tbuf[0, r] = jnp.broadcast_to(
                jnp.sum(f, axis=1, keepdims=True) * (1.0 / (sources_all * ncol)), (1, LANES)
            )
            send_row(0, tbuf, t_sem.at[0], t_sem.at[1])
        for k in range(chunks):
            col_again(k, it, u)

    acc = jnp.zeros((1, LANES), jnp.float32)
    for k in range(chunks):
        slot = (ITERS - 1) * chunks + k
        lane = pl.ds(k * chunk, chunk)
        wait_all(slot, gbuf, g_recv)
        g = (lm_ref[:, lane] * LOG2E - glane[:, lane] - jnp.log2(total_of(slot, gbuf))) * (1.0 / SCALE)
        g_ref[:, lane] = g
        acc = acc + fold(g, jnp.add)
    wait_all(0, tbuf, t_sem.at[1])
    hbuf[0, c] = total_of(0, tbuf) + jnp.broadcast_to(
        jnp.sum(acc, axis=1, keepdims=True) * (1.0 / targets_all), (1, LANES)
    )
    send_f(0, hbuf, h_sem.at[0], h_sem.at[1])
    wait_all(0, hbuf, h_sem.at[1])
    mean_ref[...] = total_of(0, hbuf)

    for copy in sent:
        copy.wait_send()
    for it in range(ITERS):
        wait_all(it, fbuf, f_send)
    for slot in range(ITERS * chunks):
        wait_all(slot, gbuf, g_send)
    wait_all(0, tbuf, t_sem.at[0])
    wait_all(0, hbuf, h_sem.at[0])


def body(nrow, ncol, src_points, tgt_points, log_src_mass, log_tgt_mass):
    sources, width = src_points.shape
    block = tgt_points.shape[0]
    targets = block * nrow
    chunks = 4
    chunk = targets // chunks
    f32 = jnp.float32
    vmem = pl.BlockSpec(memory_space=pltpu.VMEM)
    hbm = pl.BlockSpec(memory_space=pl.ANY)
    dma = pltpu.SemaphoreType.DMA
    sends = 14 if nrow == 8 else 2 * (nrow - 1)
    f, g, mean = pl.pallas_call(
        functools.partial(kernel, nrow, ncol, chunks),
        out_shape=(
            jax.ShapeDtypeStruct((1, sources), f32),
            jax.ShapeDtypeStruct((1, targets), f32),
            jax.ShapeDtypeStruct((1, LANES), f32),
        ),
        in_specs=[hbm, hbm, vmem, vmem],
        out_specs=(vmem, vmem, vmem),
        scratch_shapes=[
            pltpu.VMEM((sources, width), jnp.bfloat16),
            pltpu.VMEM((nrow, block, width), jnp.bfloat16),
            pltpu.VMEM((targets, sources), f32),
            pltpu.VMEM((1, targets), f32),
            pltpu.VMEM((1, targets), f32),
            pltpu.VMEM((3, 1, targets), f32),
            pltpu.VMEM((ITERS, ncol, 1, sources), f32),
            pltpu.VMEM((ITERS * chunks, nrow, 1, chunk), f32),
            pltpu.VMEM((1, nrow, 1, LANES), f32),
            pltpu.VMEM((1, ncol, 1, LANES), f32),
            dma((2,)),
            dma((sends,)),
            dma((nrow, 2)),
            dma((ITERS,)),
            dma((ITERS,)),
            dma((ITERS * chunks,)),
            dma((ITERS * chunks,)),
            dma((2, 1)),
            dma((2, 1)),
        ],
        compiler_params=pltpu.CompilerParams(
            collective_id=0, has_side_effects=True, vmem_limit_bytes=60 * 1024 * 1024
        ),
        name="sinkhorn",
    )(src_points, tgt_points, log_src_mass.reshape(1, -1), log_tgt_mass.reshape(1, -1))
    return f.reshape(-1), g.reshape(-1), mean[0, 0]


def solution(mesh):
    return jax.shard_map(
        functools.partial(body, mesh.shape["row"], mesh.shape["col"]),
        mesh=mesh,
        in_specs=(P("row", None), P(("col", "row"), None), P("row"), P("col")),
        out_specs=(P("row"), P("col"), P()),
        check_vma=False,
    )
```

```python
import functools
import math

import jax
import jax.numpy as jnp
from jax import lax
from jax.experimental import pallas as pl
from jax.experimental.pallas import tpu as pltpu
from jax.sharding import PartitionSpec as P

ITERS = 3
entropy_weight = 0.1
LOG2E = math.log2(math.e)
SCALE = LOG2E / entropy_weight
LANES = 128
HIGHEST = lax.Precision.HIGHEST
MESH = pl.DeviceIdType.MESH


def to_col(row):
    return jnp.broadcast_to(row, (LANES, LANES)).T


def widen(col, width):
    return jnp.concatenate([col] * (width // LANES), axis=1)


def fold(x, op):
    parts = [x[:, k : k + LANES] for k in range(0, x.shape[1], LANES)]
    while len(parts) > 1:
        parts = [op(a, b) for a, b in zip(parts[::2], parts[1::2])] + parts[len(parts) & ~1 :]
    return parts[0]


def flip(index, bit):
    return index + bit - 2 * bit * (index // bit % 2)


def kernel(
    nrow, ncol, chunks,
    x_hbm, t_hbm, ls_hbm, lm_hbm,
    f_hbm, g_hbm, mean_hbm,
    ls_ref, lm_ref, f_ref, g_ref, mean_ref, x_ref, gath, z_ref, mlane, glane, wlane, fbuf, gbuf, tbuf, hbuf,
    in_sem, out_sem, blk_send, blk_recv, f_send, f_recv, g_send, g_recv, t_sem, h_sem,
):
    r, c = lax.axis_index("row"), lax.axis_index("col")
    sources, width = x_ref.shape
    targets = z_ref.shape[0]
    block = targets // nrow
    half = block // 2
    chunk = targets // chunks
    wide, wide_first = min(512, chunk), min(256, chunk)
    sub = min(256, half)

    load_t = pltpu.make_async_copy(t_hbm, gath.at[r], in_sem.at[0])
    load_x = pltpu.make_async_copy(x_hbm, x_ref, in_sem.at[1])
    load_ls = pltpu.make_async_copy(ls_hbm, ls_ref, in_sem.at[2])
    load_lm = pltpu.make_async_copy(lm_hbm, lm_ref, in_sem.at[3])
    loads = [load_t, load_x, load_ls, load_lm]
    for copy in loads:
        copy.start()
    stores = [
        pltpu.make_async_copy(src, dst, out_sem.at[k])
        for k, (src, dst) in enumerate([(f_ref, f_hbm), (g_ref, g_hbm), (mean_ref, mean_hbm)])
    ]

    barrier = pltpu.get_barrier_semaphore()
    for d in range(1, ncol):
        pl.semaphore_signal(barrier, inc=1, device_id=(r, lax.rem(c + d, ncol)), device_id_type=MESH)
    for d in range(1, nrow):
        pl.semaphore_signal(barrier, inc=1, device_id=(lax.rem(r + d, nrow), c), device_id_type=MESH)
    load_t.wait()
    pl.semaphore_wait(barrier, nrow + ncol - 2)

    sent = []

    def send_block(slot, part, to):
        rows = pl.ds(part * half, half)
        copy = pltpu.make_async_remote_copy(
            src_ref=gath.at[slot, rows],
            dst_ref=gath.at[slot, rows],
            send_sem=blk_send.at[len(sent)],
            recv_sem=blk_recv.at[slot, part],
            device_id=(to, c),
            device_id_type=MESH,
        )
        copy.start()
        sent.append(copy)

    def wait_block(slot, part):
        rows = pl.ds(part * half, half)
        pltpu.make_async_copy(gath.at[slot, rows], gath.at[slot, rows], blk_recv.at[slot, part]).wait()

    if nrow == 8:
        p1, px, py = flip(r, 1), flip(r, 2), flip(r, 4)
        send_block(r, 0, px)
        send_block(r, 1, py)
        send_block(r, 1, px)
        send_block(r, 0, py)
        send_block(r, 0, p1)
        send_block(r, 1, p1)
    else:
        for d in range(1, nrow):
            for part in range(2):
                send_block(r, part, lax.rem(r + d, nrow))

    for copy in loads[1:]:
        copy.wait()
    x32 = x_ref[...].astype(jnp.float32)
    qx = lax.dot_general(
        jnp.ones((8, width), jnp.float32), x32 * x32, (((1,), (1,)), ((), ())),
        precision=HIGHEST, preferred_element_type=jnp.float32,
    )[0:1] * (SCALE / width)
    ls2 = ls_ref[...] * LOG2E
    els = jnp.exp2(ls2)

    def row_half(slot, part, carry):
        base = part * half

        def piece(k, carry):
            top, total = carry
            start = pl.multiple_of(slot * block + base + k * sub, sub)
            pts = gath[slot, pl.ds(pl.multiple_of(base + k * sub, sub), sub), :]
            product = lax.dot_general(
                pts, x_ref[...], (((1,), (1,)), ((), ())), preferred_element_type=jnp.float32
            )
            p32 = pts.astype(jnp.float32)
            sq = jnp.sum(p32 * p32, axis=1, keepdims=True) * (SCALE / width)
            cols = [
                to_col(lm_ref[:, pl.ds(pl.multiple_of(start + b, LANES), LANES)])
                for b in range(0, sub, LANES)
            ]
            shift = jnp.concatenate(cols, axis=0) * LOG2E - jnp.broadcast_to(sq, (sub, LANES))
            z = product * (2.0 * SCALE / width) + widen(shift, sources)
            z_ref[pl.ds(start, sub), :] = z
            new_top = jnp.maximum(top, jnp.max(z.reshape(sub // 8, 8, sources), axis=0))
            again = z_ref[pl.ds(start, sub), :].reshape(sub // 8, 8, sources)
            part = jnp.sum(jnp.exp2(again - new_top[None]), axis=0)
            return new_top, total * jnp.exp2(top - new_top) + part

        return lax.fori_loop(0, half // sub, piece, carry)

    carry = (jnp.full((8, sources), -3.0e38, jnp.float32), jnp.zeros((8, sources), jnp.float32))
    def arrived(slot, part, carry, *onward):
        wait_block(slot, part)
        for to in onward:
            send_block(slot, part, to)
        return row_half(slot, part, carry)

    carry = row_half(r, 1, row_half(r, 0, carry))
    if nrow == 8:
        carry = arrived(p1, 0, carry)
        carry = arrived(p1, 1, carry)
        wait_block(px, 0)
        send_block(px, 0, py)
        send_block(px, 0, p1)
        wait_block(py, 1)
        send_block(py, 1, px)
        send_block(py, 1, p1)
        carry = row_half(px, 0, carry)
        carry = row_half(py, 1, carry)
        px1, py1, pd = flip(px, 1), flip(py, 1), flip(px, 4)
        carry = arrived(px1, 0, carry)
        carry = arrived(px, 1, carry, p1)
        carry = arrived(py, 0, carry, p1)
        carry = arrived(py1, 1, carry)
        carry = arrived(px1, 1, carry)
        for part in range(2):
            wait_block(pd, part)
            send_block(pd, part, p1)
        carry = arrived(py1, 0, carry)
        carry = row_half(pd, 0, carry)
        carry = row_half(pd, 1, carry)
        last = flip(pd, 1)
        carry = arrived(last, 0, carry)
        carry = arrived(last, 1, carry)
    else:
        for d in range(1, nrow):
            slot = lax.rem(r + nrow - d, nrow)
            for part in range(2):
                carry = arrived(slot, part, carry)

    def send_f(k, buf, send_sem, recv_sem):
        for d in range(1, ncol):
            pltpu.make_async_remote_copy(
                src_ref=buf.at[k, c], dst_ref=buf.at[k, c], send_sem=send_sem.at[k],
                recv_sem=recv_sem.at[k], device_id=(r, lax.rem(c + d, ncol)), device_id_type=MESH,
            ).start()

    def send_row(k, buf, send_sem, recv_sem):
        for d in range(1, nrow):
            pltpu.make_async_remote_copy(
                src_ref=buf.at[k, r], dst_ref=buf.at[k, r], send_sem=send_sem.at[k],
                recv_sem=recv_sem.at[k], device_id=(lax.rem(r + d, nrow), c), device_id_type=MESH,
            ).start()

    def wait_all(k, buf, sem):
        part = buf.at[k, pl.ds(0, buf.shape[1] - 1)]
        pltpu.make_async_copy(part, part, sem.at[k]).wait()

    def total_of(k, buf):
        return functools.reduce(lambda a, b: a + b, [buf[k, d] for d in range(buf.shape[1])])

    def lse_of(k, buf):
        parts = [buf[k, d] for d in range(buf.shape[1])]
        top = functools.reduce(jnp.maximum, parts)
        return top + jnp.log2(functools.reduce(lambda a, b: a + b, [jnp.exp2(p - top) for p in parts]))

    top8, total8 = carry
    top = jnp.max(top8, axis=0, keepdims=True)
    total = jnp.sum(total8 * jnp.exp2(top8 - top), axis=0, keepdims=True)
    fbuf[0, c] = top + jnp.log2(total)
    send_f(0, fbuf, f_send, f_recv)
    wait_all(0, fbuf, f_recv)
    first_f = -lse_of(0, fbuf)
    shift = ls2 + first_f

    def sum_rows(p):
        return jnp.sum(p.T, axis=0, keepdims=True)

    def col_first(k):
        start = k * chunk

        def piece(i, unused):
            base = pl.multiple_of(i * wide_first, wide_first)
            for b in range(0, wide_first, LANES):
                rows = pl.ds(pl.multiple_of(start + base + b, LANES), LANES)
                high = jnp.max(fold(z_ref[rows, :] + shift, jnp.maximum), axis=1, keepdims=True)
                high = jnp.broadcast_to(high, (LANES, LANES))
                e = jnp.exp2(z_ref[rows, :] + shift - widen(high, sources))
                z_ref[rows, :] = e
                row = high.T[0:1, :]
                mlane[:, rows] = row
                lane = pl.ds(pl.multiple_of(base + b, LANES), LANES)
                gbuf[k, r, :, lane] = row + jnp.log2(sum_rows(fold(e, jnp.add)))
            return unused

        lax.fori_loop(0, chunk // wide_first, piece, 0)
        send_row(k, gbuf, g_send, g_recv)

    for k in range(chunks):
        col_first(k)

    def row_again(k, it, acc):
        slot = (it - 1) * chunks + k
        start = k * chunk
        lane = pl.ds(start, chunk)
        wait_all(slot, gbuf, g_recv)
        if it == 1:
            lse = lse_of(slot, gbuf)
            glane[:, lane] = lse
            wlane[0, :, lane] = jnp.exp2(mlane[:, lane] - lse)
            w = wlane[0, :, lane] * jnp.exp2(lm_ref[:, lane] * LOG2E)
            wlane[1, :, lane] = w
        else:
            w = wlane[1, :, lane] / total_of(slot, gbuf)
        wlane[2, :, lane] = w

        def piece(i, acc):
            for b in range(0, wide, LANES):
                lane = pl.ds(pl.multiple_of(start + i * wide + b, LANES), LANES)
                wc = to_col(wlane[2, :, lane])
                product = z_ref[lane, :] * widen(wc, sources)
                acc = acc + jnp.sum(product.reshape(LANES // 8, 8, sources), axis=0)
            return acc

        return lax.fori_loop(0, chunk // wide, piece, acc)

    def col_again(k, it, u):
        start = k * chunk
        slot = it * chunks + k

        def piece(i, unused):
            base = pl.multiple_of(i * wide, wide)
            for b in range(0, wide, LANES):
                rows = pl.ds(pl.multiple_of(start + base + b, LANES), LANES)
                lane = pl.ds(pl.multiple_of(base + b, LANES), LANES)
                sums = sum_rows(fold(z_ref[rows, :] * u, jnp.add))
                gbuf[slot, r, :, lane] = wlane[0, :, rows] * sums
            return unused

        lax.fori_loop(0, chunk // wide, piece, 0)
        send_row(slot, gbuf, g_send, g_recv)

    sources_all = sources * nrow
    targets_all = targets * ncol
    for it in range(1, ITERS):
        acc = jnp.zeros((8, sources), jnp.float32)
        for k in range(chunks):
            acc = row_again(k, it, acc)
        fbuf[it, c] = jnp.sum(acc, axis=0, keepdims=True)
        send_f(it, fbuf, f_send, f_recv)
        wait_all(it, fbuf, f_recv)
        rowsum = total_of(it, fbuf)
        u = els / rowsum
        if it == ITERS - 1:
            f = (first_f + qx + ls2 - jnp.log2(rowsum)) * (1.0 / SCALE)
            f_ref[...] = f
            stores[0].start()
            tbuf[0, r] = jnp.broadcast_to(
                jnp.sum(f, axis=1, keepdims=True) * (1.0 / (sources_all * ncol)), (1, LANES)
            )
            send_row(0, tbuf, t_sem.at[0], t_sem.at[1])
        for k in range(chunks):
            col_again(k, it, u)

    acc = jnp.zeros((1, LANES), jnp.float32)
    for k in range(chunks):
        slot = (ITERS - 1) * chunks + k
        lane = pl.ds(k * chunk, chunk)
        wait_all(slot, gbuf, g_recv)
        g = (lm_ref[:, lane] * LOG2E - glane[:, lane] - jnp.log2(total_of(slot, gbuf))) * (1.0 / SCALE)
        g_ref[:, lane] = g
        acc = acc + fold(g, jnp.add)
    wait_all(0, tbuf, t_sem.at[1])
    hbuf[0, c] = total_of(0, tbuf) + jnp.broadcast_to(
        jnp.sum(acc, axis=1, keepdims=True) * (1.0 / targets_all), (1, LANES)
    )
    send_f(0, hbuf, h_sem.at[0], h_sem.at[1])
    stores[1].start()
    wait_all(0, hbuf, h_sem.at[1])
    mean_ref[...] = total_of(0, hbuf)
    stores[2].start()

    for copy in sent:
        copy.wait_send()
    for it in range(ITERS):
        wait_all(it, fbuf, f_send)
    for slot in range(ITERS * chunks):
        wait_all(slot, gbuf, g_send)
    wait_all(0, tbuf, t_sem.at[0])
    wait_all(0, hbuf, h_sem.at[0])
    for copy in stores:
        copy.wait()


def body(nrow, ncol, src_points, tgt_points, log_src_mass, log_tgt_mass):
    sources, width = src_points.shape
    block = tgt_points.shape[0]
    targets = block * nrow
    chunks = 4
    chunk = targets // chunks
    f32 = jnp.float32
    hbm = pl.BlockSpec(memory_space=pl.ANY)
    dma = pltpu.SemaphoreType.DMA
    sends = 14 if nrow == 8 else 2 * (nrow - 1)
    f, g, mean = pl.pallas_call(
        functools.partial(kernel, nrow, ncol, chunks),
        out_shape=(
            jax.ShapeDtypeStruct((1, sources), f32),
            jax.ShapeDtypeStruct((1, targets), f32),
            jax.ShapeDtypeStruct((1, LANES), f32),
        ),
        in_specs=[hbm] * 4,
        out_specs=(hbm,) * 3,
        scratch_shapes=[
            pltpu.VMEM((1, sources), f32),
            pltpu.VMEM((1, targets), f32),
            pltpu.VMEM((1, sources), f32),
            pltpu.VMEM((1, targets), f32),
            pltpu.VMEM((1, LANES), f32),
            pltpu.VMEM((sources, width), jnp.bfloat16),
            pltpu.VMEM((nrow, block, width), jnp.bfloat16),
            pltpu.VMEM((targets, sources), f32),
            pltpu.VMEM((1, targets), f32),
            pltpu.VMEM((1, targets), f32),
            pltpu.VMEM((3, 1, targets), f32),
            pltpu.VMEM((ITERS, ncol, 1, sources), f32),
            pltpu.VMEM((ITERS * chunks, nrow, 1, chunk), f32),
            pltpu.VMEM((1, nrow, 1, LANES), f32),
            pltpu.VMEM((1, ncol, 1, LANES), f32),
            dma((4,)),
            dma((3,)),
            dma((sends,)),
            dma((nrow, 2)),
            dma((ITERS,)),
            dma((ITERS,)),
            dma((ITERS * chunks,)),
            dma((ITERS * chunks,)),
            dma((2, 1)),
            dma((2, 1)),
        ],
        compiler_params=pltpu.CompilerParams(
            collective_id=0, has_side_effects=True, vmem_limit_bytes=60 * 1024 * 1024
        ),
        name="sinkhorn",
    )(src_points, tgt_points, log_src_mass.reshape(1, -1), log_tgt_mass.reshape(1, -1))
    return f.reshape(-1), g.reshape(-1), mean[0, 0]


def solution(mesh):
    return jax.shard_map(
        functools.partial(body, mesh.shape["row"], mesh.shape["col"]),
        mesh=mesh,
        in_specs=(P("row", None), P(("col", "row"), None), P("row"), P("col")),
        out_specs=(P("row"), P("col"), P()),
        check_vma=False,
    )
```
